32 devices in a mesh: cap: 8 (over y, x, core), tile: 4 (over z).
Axes of the slice: x: 2, y: 2, z: 4, core: 2. Of those that a mesh axis runs over, the one named last changes fastest.
Arguments:
- load: float32 [3, 16, 1536, 128], P(None, 'cap', 'tile'), may hold values from -6 to 6
- previous: float32 [3, 16, 1536, 128], P(None, 'cap', 'tile'), may hold values from -4 to 4
- stress_old: float32 [12, 16, 1536, 128], P(None, 'cap', 'tile'), may hold values from -6 to 6
- shear_modulus: float32 [16, 1536, 128], P('cap', 'tile'), may hold values from 0.5 to 5
- relaxation: float32 [16, 1536, 128], P('cap', 'tile'), may hold values from 0.05 to 2
- density_jump: float32 [16], P('cap'), may hold values from 0.2 to 2
- element_stiffness: float32 [12, 12], replicated, may hold values from -2.9 to 3.4, as said below
- degree_slots: int32 [768], replicated, may hold values from 0 to 767, each once
Outputs:
- displacement: float32 [3, 16, 1536, 128], P(None, 'cap', 'tile')
- stress_new: float32 [12, 16, 1536, 128], P(None, 'cap', 'tile')
- potential_coeffs: float32 [768, 16, 256], P('tile', 'cap')
The draws below stay inside these ranges and needn't reach their ends.
Inputs may be any that keep to these rules, and one draw needn't show every extreme that they name: `element_stiffness`: symmetric positive definite. `degree_slots`: each degree 0 to 767 sits in exactly one slot.
All inputs are finite; a program needn't handle non-finite values.
Results may differ from the reference program's by a relative error of at most 0.00013.
Values sent between devices are 32-bit elements; how exact they have to be, the bound alone decides.
A program may use at most 128 MiB of HBM per device.

```python
import math
import jax
import jax.numpy as jnp
from jax import lax

S = 128
HRING = 1536
LDEG = 768
ITERS = 6
NR = 16


def draw_element_stiffness(key, part):
    factors = jax.random.uniform(key, (12, 12), jnp.float32, -1.7, 1.7)
    return jnp.dot(factors, factors.T) / 12.0 + 0.5 * jnp.eye(12, dtype=jnp.float32)


def steps_of(own_key, extent, pieces, smallest, top_value):
    gain, own = 1.0, jax.random.fold_in(own_key, 6)
    for dim, parts in pieces:
        steps = jnp.exp(jax.random.uniform(jax.random.fold_in(own, dim), (parts,), jnp.float32, smallest / len(pieces), top_value / len(pieces)))
        gain = gain * jnp.repeat(steps, extent[dim] // parts).reshape([-1 if axis == dim else 1 for axis in range(len(extent))])
    return gain


def bell_draw(own_key, dims, width, limit, shards=(), kind=jnp.bfloat16):
    gain = steps_of(own_key, dims, shards, -0.22, 0.18) if shards else 1.0
    drawn = jax.random.normal(own_key, dims, jnp.float32) * width * gain
    return jnp.minimum(jnp.maximum(drawn, -limit), limit).astype(kind)


def setup_inputs(seed: int = 0) -> dict:
    streams_of = jax.random.split(jax.random.key(seed), 9)
    load = bell_draw(streams_of[0], (3, NR, HRING, S), 1.0, 6.0, ((1, 8), (2, 4)), jnp.float32)
    previous = bell_draw(streams_of[1], (3, NR, HRING, S), 0.5, 4.0, ((1, 8), (2, 4)), jnp.float32)
    stress_old = bell_draw(streams_of[2], (12, NR, HRING, S), 1.0, 6.0, ((1, 8), (2, 4)), jnp.float32)
    shear_modulus = jnp.clip(jnp.exp(math.log(5.0) - 2.3025851 * jax.random.uniform(streams_of[3], (NR, HRING, S), jnp.float32) ** steps_of(streams_of[3], (NR, HRING, S), ((0, 8), (1, 4)), -0.2, 0.2)), 0.5, 5.0)
    relaxation = jnp.clip(jnp.exp(math.log(2.0) - 3.6888794 * jax.random.uniform(streams_of[4], (NR, HRING, S), jnp.float32) ** steps_of(streams_of[4], (NR, HRING, S), ((0, 8), (1, 4)), -0.2, 0.2)), 0.05, 2.0)
    density_jump = jnp.clip(jnp.exp(math.log(2.0) - 2.3025851 * jax.random.uniform(streams_of[5], (NR,), jnp.float32) ** steps_of(streams_of[5], (NR,), ((0, 8),), -0.2, 0.2)), 0.2, 2.0)
    element_stiffness = draw_element_stiffness(jax.random.fold_in(streams_of[8], 71), 0)
    degree_slots = jax.random.permutation(streams_of[7], LDEG).astype(jnp.int32)
    return dict(load=load, previous=previous, stress_old=stress_old, shear_modulus=shear_modulus, relaxation=relaxation, density_jump=density_jump, element_stiffness=element_stiffness, degree_slots=degree_slots)


precise = lax.Precision.HIGHEST
rotation_gain = 2.0
gravity_gain = 0.2

def radius_rows(offset, amount, layers):
    positions = (offset + jnp.arange(amount, dtype=jnp.int32)).astype(jnp.float32)
    return 1.0 - 0.45 * (positions + 0.5) / layers

def cycle_basis(degrees, columns):
    windings = degrees[:, None] * columns[None, :] % HRING
    angles = windings.astype(jnp.float32) * (2.0 * math.pi / HRING)
    return (jnp.cos(angles), jnp.sin(angles))

def green_kernel(degrees, target_radius, source_radius):
    degree_float = degrees.astype(jnp.float32)
    distance = jnp.abs(jnp.log(target_radius)[:, None] - jnp.log(source_radius)[None, :])
    return jnp.exp(-degree_float[:, None, None] * distance[None]) / jnp.sqrt(2.0 * degree_float + 1.0)[:, None, None]

def rotation_term(degrees, radius_list, moment):
    selector = (degrees == 2).astype(jnp.float32)
    return rotation_gain * selector[:, None, None] * (radius_list ** 2)[None, :, None] * moment[:, None, :]

def corner_values(nodal_field):
    padded = jnp.concatenate([nodal_field, jnp.zeros_like(nodal_field[:, :1])], axis=1)
    shallow = padded[:, :-1]
    deeper = padded[:, 1:]
    stacked = jnp.stack([shallow, jnp.roll(shallow, -1, axis=2), deeper, jnp.roll(deeper, -1, axis=2)], axis=1)
    return stacked.reshape((12,) + nodal_field.shape[1:])

def assemble(forces):
    grouped = forces.reshape((3, 4) + forces.shape[1:])
    shallow = grouped[:, 0] + jnp.roll(grouped[:, 1], 1, axis=2)
    deeper = grouped[:, 2] + jnp.roll(grouped[:, 3], 1, axis=2)
    moved = jnp.concatenate([jnp.zeros_like(deeper[:, :1]), deeper[:, :-1]], axis=1)
    return shallow + moved

def element_forces(nodal_field, stiffness, effective):
    return effective[None] * jnp.einsum('ab,brhs->arhs', stiffness, corner_values(nodal_field), precision=precise)

def reference(load, previous, stress_old, shear_modulus, relaxation, density_jump, element_stiffness, degree_slots):
    effective = shear_modulus / (1.0 + 0.5 * relaxation)
    carried_share = relaxation / (1.0 + 0.5 * relaxation)
    retained = (1.0 - 0.5 * relaxation) / (1.0 + 0.5 * relaxation)
    radius_all = radius_rows(0, NR, NR)
    columns = jnp.arange(HRING, dtype=jnp.int32)
    cosine, sine_table = cycle_basis(degree_slots, columns)
    weighted = previous[0] * density_jump[:, None, None]
    normalizer = math.sqrt(2.0 / HRING)
    first_half = jnp.einsum('kh,rhs->krs', cosine, weighted, precision=precise)
    second_half = jnp.einsum('kh,rhs->krs', sine_table, weighted, precision=precise)
    coefficients = jnp.concatenate([first_half, second_half], axis=2) * normalizer
    kernel = green_kernel(degree_slots, radius_all, radius_all)
    moment = jnp.einsum('j,kjs->ks', radius_all ** 4 / NR, coefficients, precision=precise)
    potential = jnp.einsum('kij,kjs->kis', kernel, coefficients, precision=precise)
    potential = potential + rotation_term(degree_slots, radius_all, moment)
    potential_field = jnp.einsum('krs,kh->rhs', potential[:, :, :S], cosine, precision=precise)
    potential_field = potential_field + jnp.einsum('krs,kh->rhs', potential[:, :, S:], sine_table, precision=precise)
    gravity_force = gravity_gain * density_jump[:, None, None] * potential_field
    right_side = load + assemble(carried_share[None] * stress_old)
    right_side = right_side + jnp.concatenate([gravity_force[None], jnp.zeros_like(load[1:])], axis=0)

    def operate(vector):
        return assemble(element_forces(vector, element_stiffness, effective))
    residual = right_side - operate(previous)
    norm_start = jnp.sum(residual * residual)

    def iterate(counter, carry_state):
        solution, residual, direction, norm_now = carry_state
        applied = operate(direction)
        step_size = norm_now / jnp.sum(direction * applied)
        solution = solution + step_size * direction
        residual = residual - step_size * applied
        norm_next = jnp.sum(residual * residual)
        direction = residual + norm_next / norm_now * direction
        return (solution, residual, direction, norm_next)
    solution = lax.fori_loop(0, ITERS, iterate, (previous, residual, residual, norm_start))[0]
    stress_new = retained[None] * stress_old + element_forces(solution, element_stiffness, effective)
    return (solution, stress_new, potential)
```

```python
import math

import jax
import jax.numpy as jnp
from jax import lax
from jax.experimental import pallas as pl
from jax.experimental.pallas import tpu as pltpu
from jax.sharding import PartitionSpec as P

HRING = 1536
LDEG = 768
ITERS = 6


precise = lax.Precision.HIGHEST
rotation_gain = 2.0
gravity_gain = 0.2


def from_behind(block, axis, distance):
    devices = range(lax.axis_size(axis))
    route = [((i - distance) % len(devices), i) for i in devices]
    return lax.ppermute(block, axis, route)


def from_behind_2(block, axis, distance):
    devices = range(lax.axis_size(axis))
    route = [(i - distance, i) for i in devices if i - distance in devices]
    return lax.ppermute(block, axis, route)


def radius_rows(offset, amount, layers):
    positions = (offset + jnp.arange(amount, dtype=jnp.int32)).astype(jnp.float32)
    return 1.0 - 0.45 * (positions + 0.5) / layers


def cycle_basis(degrees, columns):
    windings = degrees[:, None] * columns[None, :] % HRING
    angles = windings.astype(jnp.float32) * (2.0 * math.pi / HRING)
    return (jnp.cos(angles), jnp.sin(angles))


def green_kernel(degrees, target_radius, source_radius):
    degree_float = degrees.astype(jnp.float32)
    distance = jnp.abs(jnp.log(target_radius)[:, None] - jnp.log(source_radius)[None, :])
    return (
        jnp.exp(-degree_float[:, None, None] * distance[None])
        / jnp.sqrt(2.0 * degree_float + 1.0)[:, None, None]
    )


def rotation_term(degrees, radius_list, moment):
    selector = (degrees == 2).astype(jnp.float32)
    return (
        rotation_gain
        * selector[:, None, None]
        * (radius_list**2)[None, :, None]
        * moment[:, None, :]
    )


def place_corner(portion, top_pad, left_pad):
    return jnp.pad(portion, ((0, 0), (top_pad, 1 - top_pad), (left_pad, 1 - left_pad), (0, 0)))


def fold_forces(forces):
    grouped = forces.reshape((3, 4) + forces.shape[1:])
    row_count = forces.shape[1]
    col_count = forces.shape[2]
    padded_sum = place_corner(grouped[:, 0], 0, 0) + place_corner(grouped[:, 1], 0, 1)
    padded_sum = padded_sum + place_corner(grouped[:, 2], 1, 0) + place_corner(grouped[:, 3], 1, 1)
    spill_column = from_behind(padded_sum[:, :, col_count:, :], "tile", 1)
    interior = padded_sum[:, :, :col_count, :] + jnp.pad(
        spill_column, ((0, 0), (0, 0), (0, col_count - 1), (0, 0))
    )
    spill_row = from_behind_2(interior[:, row_count:], "cap", 1)
    return interior[:, :row_count] + jnp.pad(
        spill_row, ((0, 0), (0, row_count - 1), (0, 0), (0, 0))
    )


LEFT = 8
CHUNK = 16


def pair_forces(k_ref, corners, eff, c, q):
    total = k_ref[4 * c + q, 0] * corners[0]
    for b in range(1, 12):
        total = total + k_ref[4 * c + q, b] * corners[b]
    return eff * total


def load_corners(load_row, e, p):
    values = []
    for c in range(3):
        for row in (e, e + 1):
            for shift in (0, 1):
                values.append(load_row(c, row, pl.ds(p + shift, CHUNK)))
    return values


def solve_kernel(
    k_ref, prev_ref, rhs_ref, eff_ref, out_ref,
    sol, res, direc, adir, app, straight, shifted, tile_buf, cap_buf, stat,
    halo_send, halo_recv, tile_send, tile_recv, cap_send, cap_recv,
):
    caps = lax.axis_size("cap")
    tiles = lax.axis_size("tile")
    cap = lax.axis_index("cap")
    tile = lax.axis_index("tile")
    rows = prev_ref.shape[1]
    cols = prev_ref.shape[2]
    inner = pl.ds(LEFT, cols)
    mesh_ids = pl.DeviceIdType.MESH

    def clear(r, carry):
        for field in (sol, res, direc, adir, app.at[0], app.at[1]):
            for c in range(3):
                field[c, r] = jnp.zeros(field.shape[2:], jnp.float32)
        return carry

    lax.fori_loop(0, rows + 2, clear, 0)
    stat[...] = jnp.ones(stat.shape, jnp.float32)

    barrier = pltpu.get_barrier_semaphore()
    for d in range(1, tiles):
        pl.semaphore_signal(
            barrier, inc=1, device_id=(cap, lax.rem(tile + d, tiles)), device_id_type=mesh_ids
        )
    for d in range(1, caps):
        pl.semaphore_signal(
            barrier, inc=1, device_id=(lax.rem(cap + d, caps), tile), device_id_type=mesh_ids
        )
    pl.semaphore_wait(barrier, tiles + caps - 2)

    def remote(src, dst, send, recv, to_cap, to_tile):
        return pltpu.make_async_remote_copy(
            src_ref=src, dst_ref=dst, send_sem=send, recv_sem=recv,
            device_id=(to_cap, to_tile), device_id_type=mesh_ids,
        )

    def row_copies(field, kind):
        down = remote(
            field.at[:, pl.ds(rows, 1), inner], field.at[:, pl.ds(0, 1), inner],
            halo_send.at[kind, 0], halo_recv.at[kind, 0], lax.rem(cap + 1, caps), tile,
        )
        up = remote(
            field.at[:, pl.ds(1, 1), inner], field.at[:, pl.ds(rows + 1, 1), inner],
            halo_send.at[kind, 1], halo_recv.at[kind, 1], lax.rem(cap + caps - 1, caps), tile,
        )
        return down, up

    def start_rows(field, kind):
        down, up = row_copies(field, kind)

        @pl.when(cap < caps - 1)
        def _():
            down.start()

        @pl.when(cap > 0)
        def _():
            up.start()

    def wait_rows(field, kind):
        down, up = row_copies(field, kind)

        @pl.when(cap < caps - 1)
        def _():
            down.wait_send()
            up.wait_recv()

        @pl.when(cap > 0)
        def _():
            up.wait_send()
            down.wait_recv()

    def column_copies(field, kind):
        right = remote(
            field.at[:, :, pl.ds(cols, 8)], field.at[:, :, pl.ds(0, 8)],
            halo_send.at[kind, 2], halo_recv.at[kind, 2], cap, lax.rem(tile + 1, tiles),
        )
        left = remote(
            field.at[:, :, pl.ds(LEFT, 8)], field.at[:, :, pl.ds(LEFT + cols, 8)],
            halo_send.at[kind, 3], halo_recv.at[kind, 3], cap, lax.rem(tile + tiles - 1, tiles),
        )
        return right, left

    def exchange(field, kind):
        start_rows(field, kind)
        wait_rows(field, kind)
        pair = column_copies(field, kind)
        for copy in pair:
            copy.start()
        for copy in pair:
            copy.wait()

    def operate(field):
        def step(i, carry):
            p = pl.multiple_of(i * CHUNK, CHUNK)
            above = None
            for e in range(rows + 1):
                corners = load_corners(lambda c, r, d: field[c, r, d, :], e, p)
                eff = eff_ref[e, pl.ds(p, CHUNK), :]
                if e > 0:
                    for c in range(3):
                        straight[c, e - 1, pl.ds(p, CHUNK), :] = above[2 * c] + pair_forces(
                            k_ref, corners, eff, c, 0
                        )
                        shifted[c, e - 1, pl.ds(p, CHUNK), :] = above[2 * c + 1] + pair_forces(
                            k_ref, corners, eff, c, 1
                        )
                if e < rows:
                    above = [
                        pair_forces(k_ref, corners, eff, c, q) for c in range(3) for q in (2, 3)
                    ]
            return carry

        lax.fori_loop(0, (cols + 16) // CHUNK, step, 0)

    def assembled(c, r):
        return straight[c, r, inner, :] + shifted[c, r, pl.ds(LEFT - 1, cols), :]

    def fold(values):
        return jnp.sum(values.reshape((cols // 8, 8, values.shape[1])), axis=0)

    for c in range(3):
        for r in range(rows):
            sol[c, r + 1, inner, :] = prev_ref[c, r]
    exchange(sol, 2)
    operate(sol)
    for c in range(3):
        for r in range(rows):
            res[c, r + 1, inner, :] = rhs_ref[c, r] - assembled(c, r)
    exchange(res, 3)

    def iterate(k, carry):
        par = lax.rem(k, 2)
        operate(res)
        norm = jnp.zeros((8, prev_ref.shape[3]), jnp.float32)
        product = norm
        for c in range(3):
            for r in range(rows):
                applied = assembled(c, r)
                here = res[c, r + 1, inner, :]
                app[par, c, r + 1, inner, :] = applied
                norm = norm + fold(here * here)
                product = product + fold(here * applied)
        tile_buf[par, tile, 0] = norm
        tile_buf[par, tile, 1] = product
        field = app.at[par]
        tile_copies = [
            remote(
                tile_buf.at[par, tile], tile_buf.at[par, tile],
                tile_send.at[par, d - 1], tile_recv.at[par, d - 1],
                cap, lax.rem(tile + d, tiles),
            )
            for d in range(1, tiles)
        ]
        for copy in tile_copies:
            copy.start()
        start_rows(field, par)
        for copy in tile_copies:
            copy.wait()
        joined = tile_buf[par, 0]
        for t in range(1, tiles):
            joined = joined + tile_buf[par, t]
        cap_buf[par, cap] = joined
        cap_copies = [
            remote(
                cap_buf.at[par, cap], cap_buf.at[par, cap],
                cap_send.at[par, d - 1], cap_recv.at[par, d - 1],
                lax.rem(cap + d, caps), tile,
            )
            for d in range(1, caps)
        ]
        for copy in cap_copies:
            copy.start()
        wait_rows(field, par)
        pair = column_copies(field, par)
        for copy in pair:
            copy.start()
        for copy in cap_copies:
            copy.wait()
        joined = cap_buf[par, 0]
        for t in range(1, caps):
            joined = joined + cap_buf[par, t]
        sums = jnp.sum(jnp.sum(joined, axis=1, keepdims=True), axis=2, keepdims=True)
        sums = jnp.broadcast_to(sums, joined.shape)
        norm_next = sums[0]
        growth = jnp.where(k == 0, 0.0, norm_next / stat[0])
        size = norm_next / (sums[1] - growth * norm_next / stat[1])
        stat[0] = norm_next
        stat[1] = size
        growth_row = growth[:1]
        size_row = size[:1]
        for copy in pair:
            copy.wait()

        def update(r, inner_carry):
            for c in range(3):
                along = res[c, r] + growth_row * direc[c, r]
                image = app[par, c, r] + growth_row * adir[c, r]
                direc[c, r] = along
                adir[c, r] = image
                sol[c, r] = sol[c, r] + size_row * along
                res[c, r] = res[c, r] - size_row * image
            return inner_carry

        lax.fori_loop(0, rows + 2, update, 0)
        return carry

    lax.fori_loop(0, ITERS, iterate, 0)

    def emit(r, carry):
        for c in range(3):
            out_ref[c, r] = sol[c, r]
        return carry

    lax.fori_loop(0, rows + 2, emit, 0)


def solve(stiffness, previous, right_side, eff_ext):
    caps = lax.axis_size("cap")
    tiles = lax.axis_size("tile")
    _, rows, cols, sections = previous.shape
    wide = (3, rows + 2, cols + 24, sections)
    dma = pltpu.SemaphoreType.DMA
    return pl.pallas_call(
        solve_kernel,
        out_shape=jax.ShapeDtypeStruct(wide, jnp.float32),
        in_specs=[pl.BlockSpec(memory_space=pltpu.SMEM)]
        + [pl.BlockSpec(memory_space=pltpu.VMEM)] * 3,
        out_specs=pl.BlockSpec(memory_space=pltpu.VMEM),
        scratch_shapes=[pltpu.VMEM(wide, jnp.float32)] * 4
        + [pltpu.VMEM((2,) + wide, jnp.float32)]
        + [pltpu.VMEM((3, rows, cols + 24, sections), jnp.float32)] * 2
        + [
            pltpu.VMEM((2, tiles, 2, 8, sections), jnp.float32),
            pltpu.VMEM((2, caps, 2, 8, sections), jnp.float32),
            pltpu.VMEM((2, 8, sections), jnp.float32),
            dma((4, 4)),
            dma((4, 4)),
            dma((2, tiles - 1)),
            dma((2, tiles - 1)),
            dma((2, caps - 1)),
            dma((2, caps - 1)),
        ],
        compiler_params=pltpu.CompilerParams(
            collective_id=0, has_side_effects=True, vmem_limit_bytes=48 * 1024 * 1024
        ),
        name="cg_solve",
    )(stiffness, previous, right_side, eff_ext)


def stress_kernel(k_ref, sol_ref, eff_ref, relax_ref, old_ref, new_ref):
    e = pl.program_id(0) + 1
    width = old_ref.shape[2]
    base = LEFT + pl.program_id(1) * width

    def step(i, carry):
        here = pl.ds(pl.multiple_of(i * CHUNK, CHUNK), CHUNK)
        p = pl.multiple_of(base + i * CHUNK, 8)
        corners = load_corners(lambda c, r, d: sol_ref[c, r, d, :], e, p)
        eff = eff_ref[e, pl.ds(p, CHUNK), :]
        relaxation = relax_ref[0, here, :]
        retained = (1.0 - 0.5 * relaxation) / (1.0 + 0.5 * relaxation)
        for c in range(3):
            for q in range(4):
                new_ref[4 * c + q, 0, here, :] = retained * old_ref[
                    4 * c + q, 0, here, :
                ] + pair_forces(k_ref, corners, eff, c, q)
        return carry

    lax.fori_loop(0, width // CHUNK, step, 0)


def stress_update(stiffness, sol_ext, eff_ext, relaxation, stress_old):
    _, rows, cols, sections = stress_old.shape
    width = cols // 4
    block = pl.BlockSpec((12, 1, width, sections), lambda r, j: (0, r, j, 0))
    return pl.pallas_call(
        stress_kernel,
        grid=(rows, cols // width),
        out_shape=jax.ShapeDtypeStruct(stress_old.shape, jnp.float32),
        in_specs=[
            pl.BlockSpec(memory_space=pltpu.SMEM),
            pl.BlockSpec(sol_ext.shape, lambda r, j: (0, 0, 0, 0)),
            pl.BlockSpec(eff_ext.shape, lambda r, j: (0, 0, 0)),
            pl.BlockSpec((1, width, sections), lambda r, j: (r, j, 0)),
            block,
        ],
        out_specs=block,
        compiler_params=pltpu.CompilerParams(vmem_limit_bytes=32 * 1024 * 1024),
        name="stress_update",
    )(stiffness, sol_ext, eff_ext, relaxation, stress_old)


def extend_effective(effective):
    edge = from_behind(effective[:, -8:], "tile", 1)
    widened = jnp.concatenate([edge, effective, jnp.zeros_like(effective[:, :16])], axis=1)
    above = from_behind_2(widened[-1:], "cap", 1)
    return jnp.concatenate([above, widened], axis=0)


def scatter_sum(values, tile_place, slot_count):
    tiles = lax.axis_size("tile")

    def share(owner):
        return lax.dynamic_slice_in_dim(values, owner * slot_count, slot_count, 0)

    total = share(tile_place)
    for d in range(1, tiles):
        total = total + from_behind(share((tile_place + d) % tiles), "tile", d)
    return total


def body(
    load,
    previous,
    stress_old,
    shear_modulus,
    relaxation,
    density_jump,
    element_stiffness,
    degree_slots,
):
    effective = shear_modulus / (1.0 + 0.5 * relaxation)
    carried_share = relaxation / (1.0 + 0.5 * relaxation)
    eff_ext = extend_effective(effective)
    sections = load.shape[3]
    depth_rows = load.shape[1]
    cycle_cols = load.shape[2]
    cap_count = lax.axis_size("cap")
    tile_count = lax.axis_size("tile")
    layers = depth_rows * cap_count
    slot_count = LDEG // tile_count
    cap_place = lax.axis_index("cap")
    tile_place = lax.axis_index("tile")
    columns = tile_place * cycle_cols + jnp.arange(cycle_cols, dtype=jnp.int32)
    weighted = previous[0] * density_jump[:, None, None]
    normalizer = math.sqrt(2.0 / HRING)
    residual = fold_forces(carried_share[None] * stress_old) + load
    degrees = degree_slots
    cosine, sine_table = cycle_basis(degrees, columns)
    first_half = jnp.einsum("kh,rhs->krs", cosine, weighted, precision=precise)
    second_half = jnp.einsum("kh,rhs->krs", sine_table, weighted, precision=precise)
    coefficients = scatter_sum(
        jnp.concatenate([first_half, second_half], axis=2) * normalizer, tile_place, slot_count
    )
    own_degrees = lax.dynamic_slice_in_dim(degree_slots, tile_place * slot_count, slot_count, 0)
    own_radius = radius_rows(cap_place * depth_rows, depth_rows, layers)
    portion = lax.all_gather(coefficients, "cap", axis=1, tiled=True)
    source_radius = radius_rows(jnp.int32(0), portion.shape[1], layers)
    kernel = green_kernel(own_degrees, own_radius, source_radius)
    potential = jnp.einsum("kij,kjs->kis", kernel, portion, precision=precise)
    moment = jnp.einsum("j,kjs->ks", source_radius**4 / layers, portion, precision=precise)
    potential, moment = (potential, moment)
    potential = potential + rotation_term(own_degrees, own_radius, moment)
    portion = lax.all_gather(potential, "tile", axis=0, tiled=True)
    degrees = degree_slots
    cosine, sine_table = cycle_basis(degrees, columns)
    running = jnp.einsum("krs,kh->rhs", portion[:, :, :sections], cosine, precision=precise)
    surface_field = running + jnp.einsum(
        "krs,kh->rhs", portion[:, :, sections:], sine_table, precision=precise
    )
    gravity_force = gravity_gain * density_jump[:, None, None] * surface_field
    residual = residual + jnp.concatenate([gravity_force[None], jnp.zeros_like(load[1:])], axis=0)
    sol_ext = solve(element_stiffness, previous, residual, eff_ext)
    solution = sol_ext[:, 1 : depth_rows + 1, LEFT : LEFT + cycle_cols]
    stress_new = stress_update(element_stiffness, sol_ext, eff_ext, relaxation, stress_old)
    return (solution, stress_new, potential)


def solution(mesh):
    placed = (
        P(None, "cap", "tile", None),
        P(None, "cap", "tile", None),
        P(None, "cap", "tile", None),
        P("cap", "tile", None),
        P("cap", "tile", None),
        P("cap"),
        P(),
        P(),
    )
    return jax.shard_map(
        body,
        mesh=mesh,
        in_specs=placed,
        out_specs=(
            P(None, "cap", "tile", None),
            P(None, "cap", "tile", None),
            P("tile", "cap", None),
        ),
        check_vma=False,
    )
```
